32 devices in a mesh: pair: 4 (over y, x), virt: 8 (over z, core).
Axes of the slice: x: 2, y: 2, z: 4, core: 2. Of those that a mesh axis runs over, the one named last changes fastest.
Arguments:
- density_row_blocks: bfloat16 [160, 128, 2744], P('pair', 'virt'), may hold values from -6 to 6
- vir_left: bfloat16 [128, 2744], P('virt'), may hold values from -0.046875 to 0.046875
- vir_right: bfloat16 [128, 2744], P('virt'), may hold values from -0.109375 to 0.109375
- orb_energy: bfloat16 [128], P('virt'), may hold values from 0.5 to 3
- state_energy: float32 [8], replicated, may hold values from -1 to -0.1
- bra_ket_states: int32 [160, 2], P('pair'), may hold values from 0 to 7
- row_block_starts: int32 [160], P('pair'), may hold values from 0 to 2616
Outputs:
- slot_couplings: float32 [160], P('pair')
- heff: float32 [8, 8], replicated
The draws below stay inside these ranges and needn't reach their ends.
All inputs are finite; a program needn't handle non-finite values.
Results may differ from the reference program's by a relative error of at most 0.0003.
Values may be sent and summed in bfloat16 or wider, within the bound.
No kernel may reach another device: no remote copies, remote signals or barrier semaphores. Data moves between devices by JAX's collectives and lax.ppermute only.
A program may use at most 64 MiB of HBM per device.

```python
import jax
import jax.numpy as jnp
from jax import lax

MODEL_STATES = 8
ACTIVE_TRIPLES = 2744
NV = 128
BLOCK_ROW_COUNT = 128
DENSITY_BLOCKS = 160


def touch_ends(entries, stream_key, least, largest):
    longest = entries.shape.index(max(entries.shape))
    spots = []
    for shift in (0, 1):
        where = [jax.random.randint(jax.random.fold_in(stream_key, axis), (), 0, length) for axis, length in enumerate(entries.shape)]
        where[longest] = (where[longest] + shift) % entries.shape[longest]
        spots.append(tuple(where))
    return entries.at[spots[0]].set(least).at[spots[1]].set(largest)


def levels(own_key, shape, shards, low, largest):
    factor_of, own = 1.0, jax.random.fold_in(own_key, 6)
    for axis_at, blocks in shards:
        heights = jnp.exp(jax.random.uniform(jax.random.fold_in(own, axis_at), (blocks,), jnp.float32, low / len(shards), largest / len(shards)))
        factor_of = factor_of * jnp.repeat(heights, shape[axis_at] // blocks).reshape([-1 if axis == axis_at else 1 for axis in range(len(shape))])
    return factor_of


def normal_values(own_key, shape, spread, bound, shards=(), kind=jnp.bfloat16):
    drawn = jax.random.normal(own_key, shape, jnp.float32) * spread
    if len(shards) > 0:
        drawn = levels(own_key, shape, shards, -0.22, 0.18) * drawn
    return jnp.clip(drawn, min=-bound, max=bound).astype(kind)


def setup_inputs(seed: int = 0) -> dict:
    arg_keys = jax.random.split(jax.random.key(seed), 8)
    density_row_blocks = normal_values(arg_keys[0], (DENSITY_BLOCKS, BLOCK_ROW_COUNT, ACTIVE_TRIPLES), 1.0, 6.0, ((0, 4), (1, 8)))
    vir_left = normal_values(arg_keys[1], (NV, ACTIVE_TRIPLES), (BLOCK_ROW_COUNT * NV) ** -0.5, 0.046875, ((0, 8),))
    vir_right = normal_values(arg_keys[2], (NV, ACTIVE_TRIPLES), ACTIVE_TRIPLES ** -0.5, 0.109375, ((0, 8),))
    orb_energy = jnp.clip(0.5 + 2.5 * jax.random.uniform(arg_keys[3], (NV,), jnp.float32) ** levels(arg_keys[3], (NV,), ((0, 8),), -0.2, 0.2), 0.5, 3.0).astype(jnp.bfloat16)
    state_energy = jnp.clip(jax.random.uniform(arg_keys[4], (MODEL_STATES,), jnp.float32, -1.0, -0.1), -1.0, -0.1)
    bra_ket_states = touch_ends(jax.random.randint(arg_keys[5], (DENSITY_BLOCKS, 2), 0, MODEL_STATES), jax.random.fold_in(arg_keys[5], 1), 0, MODEL_STATES - 1).astype(jnp.int32)
    row_block_starts = touch_ends(jax.random.randint(arg_keys[6], (DENSITY_BLOCKS,), 0, ACTIVE_TRIPLES - BLOCK_ROW_COUNT + 1), jax.random.fold_in(arg_keys[6], 1), 0, ACTIVE_TRIPLES - BLOCK_ROW_COUNT).astype(jnp.int32)
    return dict(density_row_blocks=density_row_blocks, vir_left=vir_left, vir_right=vir_right, orb_energy=orb_energy, state_energy=state_energy, bra_ket_states=bra_ket_states, row_block_starts=row_block_starts)


def reference(density_row_blocks, vir_left, vir_right, orb_energy, state_energy, bra_ket_states, row_block_starts):
    block_rows = density_row_blocks.shape[1]
    energy = orb_energy.astype(jnp.float32)

    def single(items):
        block, couple, offset = items
        columns = lax.dynamic_slice_in_dim(vir_left, offset.astype(jnp.int32), block_rows, 1)
        contracted = jnp.dot(vir_right, block.T, preferred_element_type=jnp.float32)
        shift = state_energy[couple[0]] + state_energy[couple[1]]
        inverse = 1.0 / (energy - shift)
        return jnp.sum(columns.astype(jnp.float32) * contracted * inverse[:, None])

    couplings = lax.map(single, (density_row_blocks, bra_ket_states, row_block_starts))
    states = jnp.arange(MODEL_STATES, dtype=jnp.int32)
    first = (bra_ket_states[:, 0:1] == states[None, :]).astype(jnp.float32)
    second = (bra_ket_states[:, 1:2] == states[None, :]).astype(jnp.float32)
    coupling_sum = jnp.dot(first.T, couplings[:, None] * second, precision=lax.Precision.HIGHEST)
    heff = jnp.diag(state_energy) + 0.5 * (coupling_sum + coupling_sum.T)
    return couplings, heff
```

```python
import functools

import jax
import jax.numpy as jnp
from jax import lax
from jax.experimental import pallas as pl
from jax.experimental.pallas import tpu as pltpu
from jax.sharding import Mesh
from jax.sharding import PartitionSpec as P

LANES = 128


def rotate(x, axis, size, step):
    return lax.ppermute(x, axis, [(i, (i + step) % size) for i in range(size)])


def flip(x, axis, size, bits):
    return lax.ppermute(x, axis, [(i, i ^ bits) for i in range(size)])


def all_sum2(x, axis, size):
    bits = 1
    while bits < size:
        x = x + flip(x, axis, size, bits)
        bits *= 2
    return x


def all_sum4(x, axis, size):
    bits = 1
    while bits * 4 <= size:
        one, two, three = (flip(x, axis, size, bits * k) for k in (1, 2, 3))
        x = (x + one) + (two + three)
        bits *= 4
    while bits < size:
        x = x + flip(x, axis, size, bits)
        bits *= 2
    return x


def window_kernel(where_ref, starts_ref, left_ref, out_ref, wide_ref, *, nz, ncore, slots, rows):
    own, ntrip = left_ref.shape
    per = LANES // rows
    wide_ref[:, :ntrip] = left_ref[...].astype(jnp.float32)
    lane_group = lax.broadcasted_iota(jnp.int32, (own, LANES), 1) // rows
    my_z = where_ref[0]
    my_core = where_ref[1]

    def one(block, carry):
        step = block // ncore
        dest_z = lax.rem(my_z + step, nz)
        dest_core = lax.rem(my_core + lax.rem(block, ncore), ncore)
        shift = (dest_z * ncore + dest_core) * rows
        for group in range(-(-slots // per)):
            acc = jnp.zeros((own, LANES), jnp.float32)
            for j in range(min(per, slots - group * per)):
                at = starts_ref[group * per + j] + shift
                base = pl.multiple_of((at // LANES) * LANES, LANES)
                pair = wide_ref[:, pl.ds(base, 2 * LANES)]
                turn = lax.rem(j * rows - (at - base) + 2 * LANES, 2 * LANES)
                acc = jnp.where(lane_group == j, pltpu.roll(pair, turn, 1)[:, :LANES], acc)
            out_ref[block, :, group * LANES : (group + 1) * LANES] = acc.astype(out_ref.dtype)
        return carry

    lax.fori_loop(0, nz * ncore, one, 0)


def windows(left, starts, where, nz, ncore, rows):
    own, ntrip = left.shape
    slots = starts.shape[0]
    per = LANES // rows
    wide = (ntrip // LANES + 2) * LANES
    width = -(-slots // per) * LANES
    return pl.pallas_call(
        functools.partial(
            window_kernel, nz=nz, ncore=ncore, slots=slots, rows=rows
        ),
        out_shape=jax.ShapeDtypeStruct((nz * ncore, own, width), left.dtype),
        in_specs=[
            pl.BlockSpec(memory_space=pltpu.SMEM),
            pl.BlockSpec(memory_space=pltpu.SMEM),
            pl.BlockSpec(memory_space=pltpu.VMEM),
        ],
        out_specs=pl.BlockSpec(memory_space=pltpu.VMEM),
        scratch_shapes=[pltpu.VMEM((own, wide), jnp.float32)],
        name="windows",
    )(where, starts, left)


def couple_kernel(*refs, parts, ntrip, block):
    left_refs, right_refs = refs[:parts], refs[parts : 2 * parts]
    shift_ref, rdm_ref, out_ref, right_ref, energy_ref = refs[2 * parts :]
    at = 0
    for piece in right_refs:
        size = piece.shape[0]
        right_ref[at : at + size, :] = piece[:, :ntrip]
        energy_ref[at : at + size, :] = piece[:, ntrip : ntrip + 1].astype(jnp.float32)
        at += size
    total = rdm_ref.shape[0]
    for begin in range(0, total, block):
        cut = slice(begin, min(begin + block, total))
        contracted = lax.dot_general(
            right_ref[...],
            rdm_ref[cut, :],
            (((1,), (1,)), ((), ())),
            preferred_element_type=jnp.float32,
        )
        left = jnp.concatenate([piece[:, cut].astype(jnp.float32) for piece in left_refs], axis=0)
        inverse = 1.0 / (energy_ref[...] - shift_ref[:, cut])
        out_ref[:, cut] = jnp.sum(left * contracted * inverse, axis=0, keepdims=True)


def couple(lefts, rights, shift, rdm, block):
    total, ntrip = rdm.shape
    count = sum(piece.shape[0] for piece in rights)
    vmem = pl.BlockSpec(memory_space=pltpu.VMEM)
    return pl.pallas_call(
        functools.partial(couple_kernel, parts=len(rights), ntrip=ntrip, block=block),
        out_shape=jax.ShapeDtypeStruct((1, total), jnp.float32),
        in_specs=[vmem] * (2 * len(rights) + 2),
        out_specs=vmem,
        scratch_shapes=[
            pltpu.VMEM((count, ntrip), rdm.dtype),
            pltpu.VMEM((count, 1), jnp.float32),
        ],
        name="couple",
    )(*lefts, *rights, shift, rdm)


def local(
    density_row_blocks,
    vir_left,
    vir_right,
    orb_energy,
    state_energy,
    bra_ket_states,
    row_block_starts,
    *,
    npair,
    nz,
    ncore,
):
    slots, rows, ntrip = density_row_blocks.shape
    own = vir_right.shape[0]
    nstate = state_energy.shape[0]

    packed = jnp.concatenate([vir_right, orb_energy[:, None]], axis=1)
    right = [packed] + [rotate(packed, "z", nz, k) for k in range(1, nz)]

    where = jnp.stack([lax.axis_index("z"), lax.axis_index("core")]).astype(jnp.int32)
    cut = windows(vir_left, row_block_starts, where, nz, ncore, rows)
    cut = cut.reshape(nz, ncore, own, cut.shape[-1])
    left = [cut[0]] + [rotate(cut[k], "z", nz, k) for k in range(1, nz)]

    rights, lefts = list(right), [piece[0] for piece in left]
    if ncore > 1:
        right = jnp.concatenate(right, axis=0)
        left = jnp.stack(left)
        for k in range(1, ncore):
            rights.append(rotate(right, "core", ncore, k))
            lefts.append(rotate(left[:, k].reshape(nz * own, -1), "core", ncore, k))

    states = jnp.arange(nstate, dtype=jnp.int32)
    first = (bra_ket_states[:, 0:1] == states[None, :]).astype(jnp.float32)
    second = (bra_ket_states[:, 1:2] == states[None, :]).astype(jnp.float32)
    shift = jnp.dot(first + second, state_energy, precision=lax.Precision.HIGHEST)
    flat_rdm = density_row_blocks.reshape(slots * rows, ntrip)
    wide_shift = jnp.repeat(shift, rows)[None, :]
    sums = couple(lefts, rights, wide_shift, flat_rdm, 2 * LANES)
    partial_sums = jnp.sum(sums.reshape(slots, rows), axis=1)

    couplings = all_sum2(all_sum2(partial_sums, "core", ncore), "z", nz)
    local_sum = jnp.dot(first.T, couplings[:, None] * second, precision=lax.Precision.HIGHEST)
    coupling_sum = all_sum4(local_sum, "pair", npair)
    heff = jnp.diag(state_energy) + 0.5 * (coupling_sum + coupling_sum.T)
    return (couplings, heff)


def solution(mesh):
    npair, nvirt = mesh.shape["pair"], mesh.shape["virt"]
    ncore = 2 if nvirt % 2 == 0 else 1
    nz = nvirt // ncore
    split = Mesh(mesh.devices.reshape(npair, nz, ncore), ("pair", "z", "core"))
    virt = ("z", "core")
    placed = (
        P("pair", virt, None),
        P(virt, None),
        P(virt, None),
        P(virt),
        P(),
        P("pair", None),
        P("pair"),
    )
    return jax.shard_map(
        functools.partial(local, npair=npair, nz=nz, ncore=ncore),
        mesh=split,
        in_specs=placed,
        out_specs=(P("pair"), P()),
        check_vma=False,
    )
```

```python
import functools

import jax
import jax.numpy as jnp
from jax import lax
from jax.experimental import pallas as pl
from jax.experimental.pallas import tpu as pltpu
from jax.sharding import Mesh
from jax.sharding import PartitionSpec as P

LANES = 128
VMEM_LIMIT = 24 * 1024 * 1024


def rotate(x, axis, size, step):
    return lax.ppermute(x, axis, [(i, (i + step) % size) for i in range(size)])


def flip(x, axis, size, bits):
    return lax.ppermute(x, axis, [(i, i ^ bits) for i in range(size)])


def all_sum2(x, axis, size):
    bits = 1
    while bits < size:
        x = x + flip(x, axis, size, bits)
        bits *= 2
    return x


def all_sum4(x, axis, size):
    bits = 1
    while bits * 4 <= size:
        one, two, three = (flip(x, axis, size, bits * k) for k in (1, 2, 3))
        x = (x + one) + (two + three)
        bits *= 4
    while bits < size:
        x = x + flip(x, axis, size, bits)
        bits *= 2
    return x


def in_vmem(x):
    return pltpu.with_memory_space_constraint(x, pltpu.VMEM)


def in_hbm(x):
    return pltpu.with_memory_space_constraint(x, pltpu.HBM)


def window_kernel(
    where_ref, starts_ref, pairs_ref, state_ref, left_ref, energy_ref, *refs, nz, ncore, slots, rows
):
    out_refs, shift_ref = refs[:nz], refs[nz]
    wide_ref, window_ref = refs[nz + 1 :]
    own, ntrip = left_ref.shape
    per = LANES // rows
    span = window_ref.shape[2]
    wide_ref[:, :ntrip] = left_ref[...].astype(jnp.float32)
    for s in range(slots):
        at = starts_ref[s]
        base = pl.multiple_of((at // LANES) * LANES, LANES)
        piece = wide_ref[:, pl.ds(base, span + LANES)]
        turn = lax.rem(base - at + span + LANES, span + LANES)
        window_ref[s] = pltpu.roll(piece, turn, 1)[:, :span]

    square = lax.broadcasted_iota(jnp.int32, (own, own), 0) == lax.broadcasted_iota(
        jnp.int32, (own, own), 1
    )
    spread = jnp.broadcast_to(energy_ref[...].astype(jnp.float32), (own, own))
    energy = jnp.sum(jnp.where(square, spread, 0.0), axis=1, keepdims=True)
    energy = jnp.broadcast_to(energy, (own, LANES))

    group_of = lax.broadcasted_iota(jnp.int32, (own, LANES), 1) // rows
    my_z = where_ref[0]
    my_core = where_ref[1]
    groups = -(-slots // per)
    for k in range(nz):
        for c in range(ncore):
            dest = lax.rem(my_z + k, nz) * ncore + lax.rem(my_core + c, ncore)
            begin = dest * rows
            base = pl.multiple_of((begin // LANES) * LANES, LANES)
            turns = [lax.rem(j * rows - (begin - base) + LANES, LANES) for j in range(per)]
            for group in range(groups):
                acc = jnp.zeros((own, LANES), jnp.float32)
                for j in range(min(per, slots - group * per)):
                    piece = window_ref[group * per + j, :, pl.ds(base, LANES)]
                    acc = jnp.where(group_of == j, pltpu.roll(piece, turns[j], 1), acc)
                at = group * LANES
                out_refs[k][c, :, at : at + LANES] = acc.astype(left_ref.dtype)
            out_refs[k][c, :, groups * LANES :] = energy.astype(left_ref.dtype)

    row_group = lax.broadcasted_iota(jnp.int32, (1, LANES), 1) // rows
    for group in range(groups):
        acc = jnp.zeros((1, LANES), jnp.float32)
        for j in range(min(per, slots - group * per)):
            s = group * per + j
            acc = jnp.where(row_group == j, state_ref[pairs_ref[0, s]] + state_ref[pairs_ref[1, s]], acc)
        shift_ref[:, group * LANES : (group + 1) * LANES] = acc


def windows(left, energy, states, pairs, starts, where, nz, ncore, rows):
    own, ntrip = left.shape
    slots = starts.shape[0]
    per = LANES // rows
    span = -(-nz * ncore * rows // LANES) * LANES
    wide = -(-(ntrip + span + LANES) // LANES) * LANES
    width = -(-slots // per) * LANES
    smem = pl.BlockSpec(memory_space=pltpu.SMEM)
    vmem = pl.BlockSpec(memory_space=pltpu.VMEM)
    *cuts, shift = pl.pallas_call(
        functools.partial(window_kernel, nz=nz, ncore=ncore, slots=slots, rows=rows),
        out_shape=[
            pltpu.VMEM((ncore, own, width + LANES), left.dtype) for _ in range(nz)
        ]
        + [pltpu.VMEM((1, width), jnp.float32)],
        in_specs=[smem] * 4 + [vmem] * 2,
        out_specs=[vmem] * (nz + 1),
        scratch_shapes=[
            pltpu.VMEM((own, wide), jnp.float32),
            pltpu.VMEM((slots, own, span), jnp.float32),
        ],
        compiler_params=pltpu.CompilerParams(vmem_limit_bytes=VMEM_LIMIT),
        name="windows",
    )(where, *(in_hbm(x) for x in (starts, pairs, states, left, energy)))
    return cuts, shift


def couple_kernel(*refs, near, far, ntrip, block, slots, rows):
    left_refs, right_refs = refs[: near + far], refs[near + far : near + 2 * far + 1]
    shift_ref, source_ref, out_ref, right_ref, rdm_ref, sems = refs[near + 2 * far + 1 :]
    total = rdm_ref.shape[0]
    copies = []
    for index, begin in enumerate(range(0, total, block)):
        size = min(block, total - begin)
        copies.append(
            pltpu.make_async_copy(
                source_ref.at[pl.ds(begin, size), :],
                rdm_ref.at[pl.ds(begin, size), :],
                sems.at[index],
            )
        )
        copies[-1].start()
    at = 0
    for piece in right_refs:
        size = piece.shape[0]
        right_ref[at : at + size, :] = piece[...]
        at += size
    width = shift_ref.shape[1]

    def left_at(cut):
        pieces = [piece[0, :, cut] for piece in left_refs[:near]]
        pieces += [piece[:, cut] for piece in left_refs[near:]]
        return jnp.concatenate([piece.astype(jnp.float32) for piece in pieces], axis=0)

    energy = left_at(slice(width, width + LANES))[:, :1]
    out = jnp.zeros((8, slots), jnp.float32)
    for begin in range(0, total, block):
        end = min(begin + block, total)
        cut = slice(begin, end)
        copies[begin // block].wait()
        contracted = lax.dot_general(
            right_ref[...],
            rdm_ref[cut, :],
            (((1,), (1,)), ((), ())),
            preferred_element_type=jnp.float32,
        )
        inverse = 1.0 / (energy - shift_ref[:, cut])
        sums = jnp.sum(left_at(cut) * contracted * inverse, axis=0, keepdims=True)
        slot = (begin + lax.broadcasted_iota(jnp.int32, (end - begin, slots), 0)) // rows
        ones = (slot == lax.broadcasted_iota(jnp.int32, (end - begin, slots), 1)).astype(jnp.float32)
        out += jnp.dot(
            jnp.broadcast_to(sums, (8, end - begin)),
            ones,
            precision=lax.Precision.HIGHEST,
            preferred_element_type=jnp.float32,
        )
    out_ref[...] = out[:1]


def couple(lefts, rights, shift, rdm, near, block, slots, rows):
    total, ntrip = rdm.shape
    count = sum(piece.shape[0] for piece in rights)
    vmem = pl.BlockSpec(memory_space=pltpu.VMEM)
    args = [in_vmem(piece) for piece in (*lefts, *rights, shift)] + [in_hbm(rdm)]
    return pl.pallas_call(
        functools.partial(
            couple_kernel,
            near=near,
            far=len(rights) - 1,
            ntrip=ntrip,
            block=block,
            slots=slots,
            rows=rows,
        ),
        out_shape=pltpu.VMEM((1, slots), jnp.float32),
        in_specs=[vmem] * (len(args) - 1) + [pl.BlockSpec(memory_space=pl.ANY)],
        out_specs=vmem,
        scratch_shapes=[
            pltpu.VMEM((count, ntrip), rdm.dtype),
            pltpu.VMEM((total, ntrip), rdm.dtype),
            pltpu.SemaphoreType.DMA((-(-total // block),)),
        ],
        compiler_params=pltpu.CompilerParams(vmem_limit_bytes=VMEM_LIMIT),
        name="couple",
    )(*args)


def local(
    density_row_blocks,
    vir_left,
    vir_right,
    orb_energy,
    state_energy,
    bra_ket_states,
    row_block_starts,
    *,
    npair,
    nz,
    ncore,
):
    slots, rows, ntrip = density_row_blocks.shape
    own = vir_right.shape[0]
    nstate = state_energy.shape[0]

    right = [vir_right] + [rotate(vir_right, "z", nz, k) for k in range(1, nz)]

    where = jnp.stack([lax.axis_index("z"), lax.axis_index("core")]).astype(jnp.int32)
    cuts, shift = windows(
        vir_left,
        orb_energy[None, :],
        state_energy,
        bra_ket_states.T,
        row_block_starts,
        where,
        nz,
        ncore,
        rows,
    )
    left = [cuts[0]] + [rotate(cuts[k], "z", nz, k) for k in range(1, nz)]

    right = jnp.concatenate(right, axis=0)
    rights, lefts = [right], list(left)
    if ncore > 1:
        for k in range(1, ncore):
            rights.append(rotate(right, "core", ncore, k))
            lefts.append(
                rotate(jnp.concatenate([piece[k] for piece in left], axis=0), "core", ncore, k)
            )

    flat_rdm = density_row_blocks.reshape(slots * rows, ntrip)
    partial_sums = couple(lefts, rights, shift, flat_rdm, nz, 2 * LANES, slots, rows)
    partial_sums = partial_sums.reshape(slots)

    states = jnp.arange(nstate, dtype=jnp.int32)
    first = (bra_ket_states[:, 0:1] == states[None, :]).astype(jnp.float32)
    second = (bra_ket_states[:, 1:2] == states[None, :]).astype(jnp.float32)
    couplings = all_sum2(all_sum2(partial_sums, "core", ncore), "z", nz)
    local_sum = jnp.dot(first.T, couplings[:, None] * second, precision=lax.Precision.HIGHEST)
    coupling_sum = all_sum4(local_sum, "pair", npair)
    heff = jnp.diag(state_energy) + 0.5 * (coupling_sum + coupling_sum.T)
    return (couplings, heff)


def solution(mesh):
    npair, nvirt = mesh.shape["pair"], mesh.shape["virt"]
    ncore = 2 if nvirt % 2 == 0 else 1
    nz = nvirt // ncore
    split = Mesh(mesh.devices.reshape(npair, nz, ncore), ("pair", "z", "core"))
    virt = ("z", "core")
    placed = (
        P("pair", virt, None),
        P(virt, None),
        P(virt, None),
        P(virt),
        P(),
        P("pair", None),
        P("pair"),
    )
    return jax.shard_map(
        functools.partial(local, npair=npair, nz=nz, ncore=ncore),
        mesh=split,
        in_specs=placed,
        out_specs=(P("pair"), P()),
        check_vma=False,
    )
```

```python
import functools

import jax
import jax.numpy as jnp
from jax import lax
from jax.experimental import pallas as pl
from jax.experimental.pallas import tpu as pltpu
from jax.sharding import Mesh
from jax.sharding import PartitionSpec as P

LANES = 128
VMEM_LIMIT = 24 * 1024 * 1024


def rotate(x, axis, size, step):
    return lax.ppermute(x, axis, [(i, (i + step) % size) for i in range(size)])


def flip(x, axis, size, bits):
    return lax.ppermute(x, axis, [(i, i ^ bits) for i in range(size)])


def hop(x, axis, size, k):
    return flip(x, axis, size, k) if size & (size - 1) == 0 else rotate(x, axis, size, k)


def far_first(size):
    return sorted(range(1, size), key=lambda k: -(k & (size // 2)))


def all_sum2(x, axis, size):
    bits = 1
    while bits < size:
        x = x + flip(x, axis, size, bits)
        bits *= 2
    return x


def in_vmem(x):
    return pltpu.with_memory_space_constraint(x, pltpu.VMEM)


def in_hbm(x):
    return pltpu.with_memory_space_constraint(x, pltpu.HBM)


def window_kernel(
    where_ref, starts_ref, pairs_ref, state_ref, left_ref, energy_ref, *refs, nz, ncore, slots, rows
):
    out_refs, shift_ref = refs[:nz], refs[nz]
    wide_ref, window_ref = refs[nz + 1 :]
    own, ntrip = left_ref.shape
    per = LANES // rows
    span = window_ref.shape[2]
    wide_ref[:, :ntrip] = left_ref[...].astype(jnp.float32)
    for s in range(slots):
        at = starts_ref[s]
        base = pl.multiple_of((at // LANES) * LANES, LANES)
        piece = wide_ref[:, pl.ds(base, span + LANES)]
        turn = lax.rem(base - at + span + LANES, span + LANES)
        window_ref[s] = pltpu.roll(piece, turn, 1)[:, :span]

    square = lax.broadcasted_iota(jnp.int32, (own, own), 0) == lax.broadcasted_iota(
        jnp.int32, (own, own), 1
    )
    spread = jnp.broadcast_to(energy_ref[...].astype(jnp.float32), (own, own))
    energy = jnp.sum(jnp.where(square, spread, 0.0), axis=1, keepdims=True)
    energy = jnp.broadcast_to(energy, (own, LANES))

    group_of = lax.broadcasted_iota(jnp.int32, (own, LANES), 1) // rows
    my_z = where_ref[0]
    my_core = where_ref[1]
    groups = -(-slots // per)
    for k in range(nz):
        for c in range(ncore):
            dest_z = jnp.bitwise_xor(my_z, k) if nz & (nz - 1) == 0 else lax.rem(my_z + k, nz)
            dest = dest_z * ncore + lax.rem(my_core + c, ncore)
            begin = dest * rows
            base = pl.multiple_of((begin // LANES) * LANES, LANES)
            turns = [lax.rem(j * rows - (begin - base) + LANES, LANES) for j in range(per)]
            for group in range(groups):
                acc = jnp.zeros((own, LANES), jnp.float32)
                for j in range(min(per, slots - group * per)):
                    piece = window_ref[group * per + j, :, pl.ds(base, LANES)]
                    acc = jnp.where(group_of == j, pltpu.roll(piece, turns[j], 1), acc)
                at = group * LANES
                out_refs[k][c, :, at : at + LANES] = acc.astype(left_ref.dtype)
            out_refs[k][c, :, groups * LANES :] = energy.astype(left_ref.dtype)

    row_group = lax.broadcasted_iota(jnp.int32, (1, LANES), 1) // rows
    for group in range(groups):
        acc = jnp.zeros((1, LANES), jnp.float32)
        for j in range(min(per, slots - group * per)):
            s = group * per + j
            acc = jnp.where(row_group == j, state_ref[pairs_ref[0, s]] + state_ref[pairs_ref[1, s]], acc)
        shift_ref[:, group * LANES : (group + 1) * LANES] = acc


def windows(left, energy, states, pairs, starts, where, nz, ncore, rows):
    own, ntrip = left.shape
    slots = starts.shape[0]
    per = LANES // rows
    span = -(-nz * ncore * rows // LANES) * LANES
    wide = -(-(ntrip + span + LANES) // LANES) * LANES
    width = -(-slots // per) * LANES
    smem = pl.BlockSpec(memory_space=pltpu.SMEM)
    vmem = pl.BlockSpec(memory_space=pltpu.VMEM)
    *cuts, shift = pl.pallas_call(
        functools.partial(window_kernel, nz=nz, ncore=ncore, slots=slots, rows=rows),
        out_shape=[
            pltpu.VMEM((ncore, own, width + LANES), left.dtype) for _ in range(nz)
        ]
        + [pltpu.VMEM((1, width), jnp.float32)],
        in_specs=[smem] * 4 + [vmem] * 2,
        out_specs=[vmem] * (nz + 1),
        scratch_shapes=[
            pltpu.VMEM((own, wide), jnp.float32),
            pltpu.VMEM((slots, own, span), jnp.float32),
        ],
        compiler_params=pltpu.CompilerParams(vmem_limit_bytes=VMEM_LIMIT),
        name="windows",
    )(where, *(in_hbm(x) for x in (starts, pairs, states, left, energy)))
    return cuts, shift


def stage_kernel(source_ref, out_ref, sem):
    copy = pltpu.make_async_copy(source_ref, out_ref, sem)
    copy.start()
    copy.wait()


def stage(x):
    return pl.pallas_call(
        stage_kernel,
        out_shape=pltpu.VMEM(x.shape, x.dtype),
        in_specs=[pl.BlockSpec(memory_space=pl.ANY)],
        out_specs=pl.BlockSpec(memory_space=pltpu.VMEM),
        scratch_shapes=[pltpu.SemaphoreType.DMA],
        compiler_params=pltpu.CompilerParams(vmem_limit_bytes=VMEM_LIMIT),
        name="stage",
    )(in_hbm(x))


def couple_kernel(*refs, near, far, ntrip, block, slots, rows):
    left_refs, right_refs = refs[: near + far], refs[near + far : near + 2 * far + 1]
    shift_ref, rdm_ref, out_ref, right_ref = refs[near + 2 * far + 1 :]
    total = rdm_ref.shape[0]
    at = 0
    for piece in right_refs:
        size = piece.shape[0]
        right_ref[at : at + size, :] = piece[...]
        at += size
    width = shift_ref.shape[1]

    def left_at(cut):
        pieces = [piece[0, :, cut] for piece in left_refs[:near]]
        pieces += [piece[:, cut] for piece in left_refs[near:]]
        return jnp.concatenate([piece.astype(jnp.float32) for piece in pieces], axis=0)

    energy = left_at(slice(width, width + LANES))[:, :1]
    out = jnp.zeros((8, slots), jnp.float32)
    for begin in range(0, total, block):
        end = min(begin + block, total)
        cut = slice(begin, end)
        contracted = lax.dot_general(
            right_ref[...],
            rdm_ref[cut, :],
            (((1,), (1,)), ((), ())),
            preferred_element_type=jnp.float32,
        )
        inverse = 1.0 / (energy - shift_ref[:, cut])
        sums = jnp.sum(left_at(cut) * contracted * inverse, axis=0, keepdims=True)
        slot = (begin + lax.broadcasted_iota(jnp.int32, (end - begin, slots), 0)) // rows
        ones = (slot == lax.broadcasted_iota(jnp.int32, (end - begin, slots), 1)).astype(jnp.float32)
        out += jnp.dot(
            jnp.broadcast_to(sums, (8, end - begin)),
            ones,
            precision=lax.Precision.HIGHEST,
            preferred_element_type=jnp.float32,
        )
    out_ref[...] = out[:1]


def couple(lefts, rights, shift, rdm, near, block, slots, rows):
    total, ntrip = rdm.shape
    count = sum(piece.shape[0] for piece in rights)
    vmem = pl.BlockSpec(memory_space=pltpu.VMEM)
    args = [in_vmem(piece) for piece in (*lefts, *rights, shift, rdm)]
    return pl.pallas_call(
        functools.partial(
            couple_kernel,
            near=near,
            far=len(rights) - 1,
            ntrip=ntrip,
            block=block,
            slots=slots,
            rows=rows,
        ),
        out_shape=pltpu.VMEM((1, slots), jnp.float32),
        in_specs=[vmem] * len(args),
        out_specs=vmem,
        scratch_shapes=[pltpu.VMEM((count, ntrip), rdm.dtype)],
        compiler_params=pltpu.CompilerParams(vmem_limit_bytes=VMEM_LIMIT),
        name="couple",
    )(*args)


def local(
    density_row_blocks,
    vir_left,
    vir_right,
    orb_energy,
    state_energy,
    bra_ket_states,
    row_block_starts,
    *,
    npair,
    nz,
    ncore,
):
    slots, rows, ntrip = density_row_blocks.shape
    own = vir_right.shape[0]
    nstate = state_energy.shape[0]

    flat_rdm = stage(density_row_blocks.reshape(slots * rows, ntrip))
    right = [vir_right] + [hop(vir_right, "z", nz, k) for k in far_first(nz)]

    where = jnp.stack([lax.axis_index("z"), lax.axis_index("core")]).astype(jnp.int32)
    cuts, shift = windows(
        vir_left,
        orb_energy[None, :],
        state_energy,
        bra_ket_states.T,
        row_block_starts,
        where,
        nz,
        ncore,
        rows,
    )
    left = [cuts[0]] + [hop(cuts[k], "z", nz, k) for k in far_first(nz)]

    right[0], flat_rdm = lax.optimization_barrier((right[0], flat_rdm))
    right = jnp.concatenate(right, axis=0)
    rights, lefts = [right], list(left)
    if ncore > 1:
        for k in range(1, ncore):
            rights.append(rotate(right, "core", ncore, k))
            lefts.append(
                rotate(jnp.concatenate([piece[k] for piece in left], axis=0), "core", ncore, k)
            )

    partial_sums = couple(lefts, rights, shift, flat_rdm, nz, 2 * LANES, slots, rows)
    partial_sums = partial_sums.reshape(slots)

    states = jnp.arange(nstate, dtype=jnp.int32)
    first = (bra_ket_states[:, 0:1] == states[None, :]).astype(jnp.float32)
    second = (bra_ket_states[:, 1:2] == states[None, :]).astype(jnp.float32)
    couplings = all_sum2(all_sum2(partial_sums, "core", ncore), "z", nz)
    local_sum = jnp.dot(first.T, couplings[:, None] * second, precision=lax.Precision.HIGHEST)
    coupling_sum = all_sum2(local_sum, "pair", npair)
    heff = jnp.diag(state_energy) + 0.5 * (coupling_sum + coupling_sum.T)
    return (couplings, heff)


def solution(mesh):
    npair, nvirt = mesh.shape["pair"], mesh.shape["virt"]
    ncore = 2 if nvirt % 2 == 0 else 1
    nz = nvirt // ncore
    split = Mesh(mesh.devices.reshape(npair, nz, ncore), ("pair", "z", "core"))
    virt = ("z", "core")
    placed = (
        P("pair", virt, None),
        P(virt, None),
        P(virt, None),
        P(virt),
        P(),
        P("pair", None),
        P("pair"),
    )
    return jax.shard_map(
        functools.partial(local, npair=npair, nz=nz, ncore=ncore),
        mesh=split,
        in_specs=placed,
        out_specs=(P("pair"), P()),
        check_vma=False,
    )
```
